32 devices in a mesh: dp: 8 (over z, y), rep: 4 (over x, core).
Axes of the slice: x: 2, y: 2, z: 4, core: 2. Of those that a mesh axis runs over, the one named last changes fastest.
Arguments:
- enc: bfloat16 [64, 48, 640], P(('dp', 'rep')), may hold values from -6 to 6
- pred: bfloat16 [64, 17, 640], P(('dp', 'rep')), may hold values from -6 to 6
- labels: int32 [64, 16], P(('dp', 'rep')), may hold values from 1 to 4095
- frame_len: int32 [64], P(('dp', 'rep')), may hold values from 24 to 48, as said below
- label_len: int32 [64], P(('dp', 'rep')), may hold values from 1 to 16, as said below
- w_enc: bfloat16 [640, 640], replicated, may hold values from -0.25 to 0.25
- w_pred: bfloat16 [640, 640], replicated, may hold values from -0.25 to 0.25
- b_joint: bfloat16 [640], replicated, may hold values from -3 to 3
- w_out: bfloat16 [640, 4096], replicated, may hold values from -0.69921875 to 0.69921875
- b_out: bfloat16 [4096], replicated, may hold values from -5 to 5
Outputs:
- step_enc: float32 [640, 640], replicated
- step_pred: float32 [640, 640], replicated
- step_out: float32 [640, 4096], replicated
- step_bias_out: float32 [4096], replicated
- step_bias_joint: float32 [640], replicated
- mean_loss: float32 [], replicated
The draws below stay inside these ranges and needn't reach their ends.
Inputs may be any that keep to these rules, and one draw needn't show every extreme that they name: `frame_len`: the last utterance has all 48 frames. `label_len`: the last utterance has all 16 labels.
All inputs are finite; a program needn't handle non-finite values.
Results may differ from the reference program's by a relative error of at most 0.0055.
Values sent between devices are 32-bit elements; how exact they have to be, the bound alone decides.
A program may use at most 256 MiB of HBM per device.

```python
import jax
import jax.numpy as jnp
from jax import lax

ENC_DIM = 640
PRED_DIM = 640
JOINT = 640
VOCAB = 4096
FRAMES = 48
LABELS = 16
BATCH = 64


def draw_frame_len(key, part):
    positions = jnp.arange(BATCH, dtype=jnp.int32)
    picked = jax.random.randint(jax.random.fold_in(key, 11), (BATCH,), FRAMES // 2, FRAMES + 1)
    return jnp.where(positions == BATCH - 1, FRAMES, picked).astype(jnp.int32)


def draw_label_len(key, part):
    positions = jnp.arange(BATCH, dtype=jnp.int32)
    baseline = LABELS * (BATCH + 2 * positions) // (3 * BATCH)
    jitter = jax.random.randint(jax.random.fold_in(key, 23), (BATCH,), -1, 2)
    lengths = jnp.clip(baseline + jitter, 1, LABELS)
    return jnp.where(positions == BATCH - 1, LABELS, lengths).astype(jnp.int32)


def place_ends(drawn, stream_key, least, top_value):
    place = [jax.random.randint(jax.random.fold_in(stream_key, axis), (), 0, length) for axis, length in enumerate(drawn.shape)]
    main_axis = drawn.shape.index(max(drawn.shape))
    neighbour = place[:main_axis] + [(place[main_axis] + 1) % drawn.shape[main_axis]] + place[main_axis + 1:]
    return drawn.at[tuple(place)].set(least).at[tuple(neighbour)].set(top_value)


def level_of(rng, shape, cuts, smallest, high):
    level = 1.0
    for axis_at, shards_of in cuts:
        steps = jax.random.uniform(jax.random.fold_in(jax.random.fold_in(rng, 6), axis_at), (shards_of,), jnp.float32, smallest / len(cuts), high / len(cuts))
        level = level * jnp.repeat(jnp.exp(steps), shape[axis_at] // shards_of).reshape((-1,) + (1,) * (len(shape) - 1 - axis_at))
    return level


def gaussian(stream_key, shape, width, limit, split=(), held_as=jnp.bfloat16):
    factor_of = level_of(stream_key, shape, split, -0.22, 0.18) if split else 1.0
    result = jax.random.normal(stream_key, shape, jnp.float32) * width * factor_of
    return jnp.minimum(jnp.maximum(result, -limit), limit).astype(held_as)


def setup_inputs(seed: int = 0) -> dict:
    seeds = jax.random.split(jax.random.key(seed), 11)
    return {
        "enc": gaussian(seeds[0], (BATCH, FRAMES, ENC_DIM), 1.0, 6.0, ((0, 32),)),
        "pred": gaussian(seeds[1], (BATCH, LABELS + 1, PRED_DIM), 1.0, 6.0, ((0, 32),)),
        "labels": place_ends(jax.random.randint(seeds[2], (BATCH, LABELS), 1, VOCAB), jax.random.fold_in(seeds[2], 1), 1, VOCAB - 1).astype(jnp.int32),
        "frame_len": draw_frame_len(jax.random.fold_in(seeds[10], 71), 0),
        "label_len": draw_label_len(jax.random.fold_in(seeds[10], 71), 0),
        "w_enc": gaussian(seeds[5], (ENC_DIM, JOINT), ENC_DIM ** -0.5, 0.25),
        "w_pred": gaussian(seeds[6], (PRED_DIM, JOINT), PRED_DIM ** -0.5, 0.25),
        "b_joint": gaussian(seeds[7], (JOINT,), 0.5, 3.0),
        "w_out": gaussian(seeds[8], (JOINT, VOCAB), 0.12, 0.69921875),
        "b_out": gaussian(seeds[9], (VOCAB,), 1.0, 5.0),
    }


NEG = -1e+30
EPS = 1e-06

def forward_rows(blank, emit):
    count_labels = blank.shape[1]
    positions = jnp.arange(count_labels, dtype=jnp.int32)

    def along_labels(carry_left, inputs):
        top_term, emit_here = inputs
        cell_value = jnp.logaddexp(top_term, carry_left)
        return (cell_value + emit_here, cell_value)

    def along_frames(top_row, inputs):
        blank_row, emit_row = inputs
        unused_carry, alpha_row = lax.scan(along_labels, jnp.float32(NEG), (top_row, emit_row))
        return (alpha_row + blank_row, alpha_row)
    first_top = jnp.where(positions == 0, 0.0, NEG).astype(jnp.float32)
    unused_last, alpha = lax.scan(along_frames, first_top, (blank, emit))
    return alpha

def backward_rows(blank, emit, frame_count, label_count):
    num_frames, count_labels = blank.shape
    positions = jnp.arange(count_labels, dtype=jnp.int32)
    neg_row = jnp.full((count_labels,), NEG, jnp.float32)
    terminal = jnp.where(positions == label_count, 0.0, NEG).astype(jnp.float32)

    def along_labels_back(carry_right, inputs):
        below_value, blank_here, emit_here, live = inputs
        cell_value = jnp.logaddexp(below_value + blank_here, carry_right + emit_here)
        cell_value = jnp.where(live, cell_value, NEG).astype(jnp.float32)
        return (cell_value, cell_value)

    def along_frames_back(carry_below, inputs):
        frame_pos, blank_row, emit_row = inputs
        below = jnp.where(frame_pos == frame_count - 1, terminal, jnp.where(frame_pos >= frame_count, neg_row, carry_below))
        live = (positions <= label_count) & (frame_pos < frame_count)
        unused_carry, beta_row = lax.scan(along_labels_back, jnp.float32(NEG), (below, blank_row, emit_row, live), reverse=True)
        return (beta_row, (beta_row, below))
    frame_ids = jnp.arange(num_frames, dtype=jnp.int32)
    unused_last, (beta, below) = lax.scan(along_frames_back, neg_row, (frame_ids, blank, emit), reverse=True)
    return (beta, below)

def utterance_terms(enc_row, pred_row, label_row, frame_count, label_count, w_enc, w_pred, b_joint, w_out, b_out):
    num_frames = enc_row.shape[0]
    count_labels = pred_row.shape[0]
    joint_width = w_enc.shape[1]
    vocab_size = w_out.shape[1]
    enc_proj = jnp.dot(enc_row, w_enc, preferred_element_type=jnp.float32)
    pred_proj = jnp.dot(pred_row, w_pred, preferred_element_type=jnp.float32) + b_joint.astype(jnp.float32)
    hidden = jnp.tanh(enc_proj[:, None, :] + pred_proj[None, :, :]).astype(jnp.bfloat16)
    hidden = lax.optimization_barrier(hidden.reshape(num_frames * count_labels, joint_width))
    logits = jnp.dot(hidden, w_out, preferred_element_type=jnp.float32) + b_out.astype(jnp.float32)
    log_probs = jax.nn.log_softmax(logits, axis=-1)
    targets = jnp.concatenate([label_row.astype(jnp.int32), jnp.ones((1,), jnp.int32)])
    target_cols = jnp.tile(targets, num_frames)
    vocab_pos = jnp.arange(vocab_size, dtype=jnp.int32)
    is_target = vocab_pos[None, :] == target_cols[:, None]
    emit = lax.optimization_barrier(jnp.sum(jnp.where(is_target, log_probs, 0.0), axis=1)).reshape(num_frames, count_labels)
    blank = log_probs[:, 0].reshape(num_frames, count_labels)
    alpha = forward_rows(blank, emit)
    beta, below = backward_rows(blank, emit, frame_count, label_count)
    log_total = beta[0, 0]
    right = jnp.concatenate([beta[:, 1:], jnp.full((num_frames, 1), NEG, jnp.float32)], axis=1)
    blank_occ = jnp.exp(alpha + blank + below - log_total).reshape(-1)
    emit_occ = jnp.exp(alpha + emit + right - log_total).reshape(-1)
    probs = jnp.exp(log_probs)
    grad_logits = probs * (blank_occ + emit_occ)[:, None]
    grad_logits = grad_logits - jnp.where(vocab_pos[None, :] == 0, blank_occ[:, None], 0.0)
    grad_logits = grad_logits - jnp.where(is_target, emit_occ[:, None], 0.0)
    grad_logits = lax.optimization_barrier(grad_logits.astype(jnp.bfloat16))
    grad_out = lax.dot_general(hidden, grad_logits, (((0,), (0,)), ((), ())), preferred_element_type=jnp.float32)
    grad_bias_out = lax.optimization_barrier(jnp.sum(grad_logits.astype(jnp.float32), axis=0))
    grad_hidden = lax.dot_general(grad_logits, w_out, (((1,), (1,)), ((), ())), preferred_element_type=jnp.float32)
    hidden_wide = hidden.astype(jnp.float32)
    grad_pre = (grad_hidden * (1.0 - hidden_wide * hidden_wide)).reshape(num_frames, count_labels, joint_width)
    grad_enc_proj = lax.optimization_barrier(lax.optimization_barrier(jnp.sum(grad_pre, axis=1)).astype(jnp.bfloat16))
    grad_pred_proj = lax.optimization_barrier(lax.optimization_barrier(jnp.sum(grad_pre, axis=0)).astype(jnp.bfloat16))
    grad_enc = lax.dot_general(enc_row, grad_enc_proj, (((0,), (0,)), ((), ())), preferred_element_type=jnp.float32)
    grad_pred = lax.dot_general(pred_row, grad_pred_proj, (((0,), (0,)), ((), ())), preferred_element_type=jnp.float32)
    grad_bias_joint = lax.optimization_barrier(jnp.sum(grad_pred_proj.astype(jnp.float32), axis=0))
    return (-log_total, (grad_enc, grad_pred, grad_out, grad_bias_out, grad_bias_joint))

def local_sums(enc, pred, labels, frame_len, label_len, w_enc, w_pred, b_joint, w_out, b_out):
    initial = (jnp.zeros(w_enc.shape, jnp.float32), jnp.zeros(w_pred.shape, jnp.float32), jnp.zeros(w_out.shape, jnp.float32), jnp.zeros(b_out.shape, jnp.float32), jnp.zeros(b_joint.shape, jnp.float32))

    def one_utterance(carry, inputs):
        loss_sum, grad_sums = carry
        enc_row, pred_row, label_row, frame_count, label_count = inputs
        loss_one, grads_one = utterance_terms(enc_row, pred_row, label_row, frame_count, label_count, w_enc, w_pred, b_joint, w_out, b_out)
        added = tuple((total + term for total, term in zip(grad_sums, grads_one)))
        return ((loss_sum + loss_one, added), None)
    (loss_sum, grads), unused_ys = lax.scan(one_utterance, (jnp.float32(0.0), initial), (enc, pred, labels, frame_len, label_len))
    return (loss_sum, grads)

def reference(enc, pred, labels, frame_len, label_len, w_enc, w_pred, b_joint, w_out, b_out):
    loss_sum, grads = local_sums(enc, pred, labels, frame_len, label_len, w_enc, w_pred, b_joint, w_out, b_out)
    param_count = sum((int(item.size) for item in grads))
    total_sq = jnp.float32(0.0)
    for item in grads:
        total_sq = total_sq + jnp.sum(item * item)
    scale = lax.rsqrt(total_sq / jnp.float32(param_count) + EPS)
    label_total = jnp.sum(label_len).astype(jnp.float32)
    return (grads[0] * scale, grads[1] * scale, grads[2] * scale, grads[3] * scale, grads[4] * scale, loss_sum / label_total)
```

```python
import functools

import jax
import jax.numpy as jnp
from jax import lax
from jax.experimental import pallas as pl
from jax.experimental.pallas import tpu as pltpu
from jax.sharding import PartitionSpec as P

NEG = -1e30
EPS = 1e-06
LANES = 128
VMEM_LIMIT = 60 * 1024 * 1024


def row_stats_kernel(chunk, hidden_ref, w_ref, bias_ref, target_ref, out_ref, logits_ref):
    rows = hidden_ref.shape[0]
    vocab = w_ref.shape[1]
    target = target_ref[...]
    lane = lax.broadcasted_iota(jnp.int32, (rows, chunk), 1)

    def folded(op, tile):
        total = tile[:, :LANES]
        for start in range(LANES, chunk, LANES):
            total = op(total, tile[:, start : start + LANES])
        return total

    def logits_step(step, carry):
        top, picked = carry
        base = pl.multiple_of(step * chunk, chunk)
        tile = jnp.dot(
            hidden_ref[...], w_ref[:, pl.ds(base, chunk)], preferred_element_type=jnp.float32
        )
        tile = tile + bias_ref[:, pl.ds(base, chunk)]
        logits_ref[:, pl.ds(base, chunk)] = tile
        top = jnp.maximum(top, folded(jnp.maximum, tile))
        hit = jnp.where(lane == target - base, tile, 0.0)
        return top, picked + folded(jnp.add, hit)

    start = (
        jnp.full((rows, LANES), NEG, jnp.float32),
        jnp.zeros((rows, LANES), jnp.float32),
    )
    top, picked = lax.fori_loop(0, vocab // chunk, logits_step, start)
    top = jnp.max(top, axis=1, keepdims=True)
    emit = jnp.sum(picked, axis=1, keepdims=True)

    def exp_step(step, total):
        base = pl.multiple_of(step * chunk, chunk)
        return total + folded(jnp.add, jnp.exp(logits_ref[:, pl.ds(base, chunk)] - top))

    total = lax.fori_loop(0, vocab // chunk, exp_step, jnp.zeros((rows, LANES), jnp.float32))
    denominator = top + jnp.log(jnp.sum(total, axis=1, keepdims=True))
    blank = logits_ref[:, 0:1]
    column = lax.broadcasted_iota(jnp.int32, (rows, LANES), 1)
    out_ref[...] = jnp.where(
        column == 0,
        denominator,
        jnp.where(column == 1, blank - denominator, emit - denominator),
    )


def row_stats(hidden, w_out, bias, target):
    rows, width = hidden.shape
    vocab = w_out.shape[1]
    tile = rows // 8
    return pl.pallas_call(
        functools.partial(row_stats_kernel, 512),
        grid=(rows // tile,),
        out_shape=jax.ShapeDtypeStruct((rows, LANES), jnp.float32),
        in_specs=[
            pl.BlockSpec((tile, width), lambda i: (i, 0)),
            pl.BlockSpec((width, vocab), lambda i: (0, 0)),
            pl.BlockSpec((1, vocab), lambda i: (0, 0)),
            pl.BlockSpec((tile, 1), lambda i: (i, 0)),
        ],
        out_specs=pl.BlockSpec((tile, LANES), lambda i: (i, 0)),
        scratch_shapes=[pltpu.VMEM((tile, vocab), jnp.float32)],
        compiler_params=pltpu.CompilerParams(
            dimension_semantics=("arbitrary",), vmem_limit_bytes=VMEM_LIMIT
        ),
        name="row_stats",
    )(hidden, w_out, bias, target)


def lattice_kernel(
    frames,
    slots,
    group,
    blank_ref,
    emit_ref,
    frame_ref,
    label_ref,
    blank_occ_ref,
    emit_occ_ref,
    loss_ref,
    alpha_diag,
    beta_diag,
    blank_diag,
    emit_diag,
    base_diag,
):
    lead = slots - 1
    diags = frames + slots - 1

    def slot_of(rows):
        return lax.broadcasted_iota(jnp.int32, (rows, LANES), 1) % group

    slot = slot_of(diags)
    frame = lax.broadcasted_iota(jnp.int32, (diags, LANES), 0) - slot
    count = frame_ref[...]
    label = label_ref[...]
    blank_skew = jnp.full((diags, LANES), NEG, jnp.float32)
    emit_skew = jnp.full((diags, LANES), NEG, jnp.float32)
    for u in range(slots):
        here = slot == u
        blank_skew = jnp.where(here, blank_ref[pl.ds(lead - u, diags), :], blank_skew)
        emit_skew = jnp.where(here, emit_ref[pl.ds(lead - u, diags), :], emit_skew)
    blank_diag[...] = blank_skew
    emit_diag[...] = emit_skew
    base_diag[...] = jnp.where((frame == count - 1) & (slot == label), 0.0, NEG)
    beta_diag[...] = jnp.full(beta_diag.shape, NEG, jnp.float32)
    row_slot = slot_of(1)
    first = row_slot == 0
    last = row_slot == lead
    alpha = jnp.where(first, 0.0, NEG)
    alpha_diag[0:1, :] = alpha
    beta = jnp.full((1, LANES), NEG, jnp.float32)

    def joined(left, right):
        top = jnp.maximum(left, right)
        return top + jnp.log1p(jnp.exp(-jnp.abs(left - right)))

    for step in range(diags):
        back = diags - 1 - step
        back_frame = back - row_slot
        below = jnp.where(back_frame < count - 1, beta, base_diag[back : back + 1, :])
        after = jnp.where(last, NEG, pltpu.roll(beta, LANES - 1, 1))
        beta = joined(below + blank_diag[back : back + 1, :], after + emit_diag[back : back + 1, :])
        live = (row_slot <= label) & (back_frame < count) & (back_frame >= 0)
        beta = jnp.where(live, beta, NEG)
        beta_diag[back : back + 1, :] = beta
        if step:
            prev = step - 1
            above = alpha + blank_diag[prev : prev + 1, :]
            left = pltpu.roll(alpha + emit_diag[prev : prev + 1, :], 1, 1)
            alpha = joined(above, jnp.where(first, NEG, left))
            step_frame = step - row_slot
            alpha = jnp.where((step_frame >= 0) & (step_frame < frames), alpha, NEG)
            alpha_diag[step : step + 1, :] = alpha

    grid_slot = slot_of(frames)
    grid_frame = lax.broadcasted_iota(jnp.int32, (frames, LANES), 0)
    neg_grid = jnp.full((frames, LANES), NEG, jnp.float32)
    alpha_grid, beta_grid, next_grid = neg_grid, neg_grid, neg_grid
    for u in range(slots):
        here = grid_slot == u
        alpha_grid = jnp.where(here, alpha_diag[pl.ds(u, frames), :], alpha_grid)
        beta_grid = jnp.where(here, beta_diag[pl.ds(u, frames), :], beta_grid)
        next_grid = jnp.where(here, beta_diag[pl.ds(u + 1, frames), :], next_grid)
    terminal = jnp.where((grid_frame == count - 1) & (grid_slot == label), 0.0, NEG)
    below = jnp.where(grid_frame < count - 1, next_grid, terminal)
    right = jnp.where(grid_slot == lead, NEG, pltpu.roll(beta_grid, LANES - 1, 1))
    lane = lax.broadcasted_iota(jnp.int32, (1, LANES), 1)
    total = jnp.zeros((1, LANES), jnp.float32)
    for start in range(0, LANES, group):
        total = jnp.where(lane // group == start // group, beta_grid[0:1, start : start + 1], total)
    blank = blank_ref[pl.ds(lead, frames), :]
    emit = emit_ref[pl.ds(lead, frames), :]
    used = grid_slot < slots
    blank_occ_ref[...] = jnp.where(used, jnp.exp(alpha_grid + blank + below - total), 0.0)
    emit_occ_ref[...] = jnp.where(used, jnp.exp(alpha_grid + emit + right - total), 0.0)
    loss_ref[...] = jnp.broadcast_to(-total, loss_ref.shape)


def lattice(blank, emit, frame_len, label_len):
    utterances, slots, frames = blank.shape
    group = LANES // utterances
    diags = frames + slots - 1

    def packed(grid):
        by_frame = jnp.transpose(grid, (2, 0, 1))
        by_frame = jnp.pad(
            by_frame, ((slots - 1, slots - 1), (0, 0), (0, group - slots)), constant_values=NEG
        )
        return by_frame.reshape(frames + 2 * slots - 2, utterances * group)

    def spread(lengths):
        return jnp.repeat(lengths, group)[None, :]

    diag_rows = (diags + 8) // 8 * 8
    blank_occ, emit_occ, loss = pl.pallas_call(
        functools.partial(lattice_kernel, frames, slots, group),
        out_shape=(
            jax.ShapeDtypeStruct((frames, LANES), jnp.float32),
            jax.ShapeDtypeStruct((frames, LANES), jnp.float32),
            jax.ShapeDtypeStruct((8, LANES), jnp.float32),
        ),
        scratch_shapes=[pltpu.VMEM((diag_rows, LANES), jnp.float32)] * 2
        + [pltpu.VMEM((diags, LANES), jnp.float32)] * 3,
        name="lattice",
    )(packed(blank), packed(emit), spread(frame_len), spread(label_len))

    def unpacked(grid):
        grid = grid.reshape(frames, utterances, group)[:, :, :slots]
        return jnp.transpose(grid, (1, 2, 0))

    return unpacked(blank_occ), unpacked(emit_occ), loss[0, ::group]


def backward_kernel(
    utterances,
    slots,
    frames,
    row_tile,
    hidden_ref,
    turned_ref,
    w_ref,
    bias_ref,
    target_ref,
    cell_ref,
    grad_out_ref,
    grad_bias_ref,
    enc_ref,
    pred_ref,
    dlogits_ref,
    dhidden_ref,
):
    step = pl.program_id(0)
    rows = hidden_ref.shape[0]
    tile = w_ref.shape[1]
    base = step * tile

    @pl.when(step == 0)
    def start():
        dhidden_ref[...] = jnp.zeros(dhidden_ref.shape, jnp.float32)

    column = lax.broadcasted_iota(jnp.int32, (row_tile, tile), 1) + base

    def row_step(index, bias_sum):
        at = pl.ds(pl.multiple_of(index * row_tile, row_tile), row_tile)
        logits = jnp.dot(hidden_ref[at, :], w_ref[...], preferred_element_type=jnp.float32)
        cell = cell_ref[at, :]
        log_probs = (logits + bias_ref[...]) - cell[:, 0:1]
        grad = jnp.exp(log_probs) * (cell[:, 1:2] + cell[:, 2:3])
        grad = grad - jnp.where(column == 0, cell[:, 1:2], 0.0)
        grad = grad - jnp.where(column == target_ref[at, :], cell[:, 2:3], 0.0)
        grad = grad.astype(jnp.bfloat16)
        dlogits_ref[at, :] = grad
        dhidden_ref[at, :] += lax.dot_general(
            grad, w_ref[...], (((1,), (1,)), ((), ())), preferred_element_type=jnp.float32
        )
        return bias_sum + jnp.sum(grad.astype(jnp.float32), axis=0, keepdims=True)

    grad_bias_ref[...] = lax.fori_loop(
        0, rows // row_tile, row_step, jnp.zeros((1, tile), jnp.float32)
    )
    grad_out_ref[...] = jnp.dot(
        turned_ref[...], dlogits_ref[...], preferred_element_type=jnp.float32
    )

    @pl.when(step == pl.num_programs(0) - 1)
    def finish():
        for b in range(utterances):
            enc_sum = jnp.zeros(enc_ref.shape[1:], jnp.float32)
            for u in range(slots):
                at = pl.ds((b * slots + u) * frames, frames)
                wide = hidden_ref[at, :].astype(jnp.float32)
                grad_pre = dhidden_ref[at, :] * (1.0 - wide * wide)
                enc_sum = enc_sum + grad_pre
                pred_ref[b, u : u + 1, :] = jnp.sum(grad_pre, axis=0, keepdims=True)
            enc_ref[b] = enc_sum


def backward(hidden, turned, w_out, bias, target, cells, utterances, slots, frames):
    rows, width = hidden.shape
    vocab = w_out.shape[1]
    tile = 512
    whole = lambda i: (0, 0)
    across = lambda i: (0, i)
    return pl.pallas_call(
        functools.partial(backward_kernel, utterances, slots, frames, rows // 4),
        grid=(vocab // tile,),
        out_shape=(
            jax.ShapeDtypeStruct((width, vocab), jnp.float32),
            jax.ShapeDtypeStruct((1, vocab), jnp.float32),
            jax.ShapeDtypeStruct((utterances, frames, width), jnp.float32),
            jax.ShapeDtypeStruct((utterances, slots, width), jnp.float32),
        ),
        in_specs=[
            pl.BlockSpec((rows, width), whole),
            pl.BlockSpec((width, rows), whole),
            pl.BlockSpec((width, tile), across),
            pl.BlockSpec((1, tile), across),
            pl.BlockSpec((rows, 1), whole),
            pl.BlockSpec((rows, LANES), whole),
        ],
        out_specs=(
            pl.BlockSpec((width, tile), across),
            pl.BlockSpec((1, tile), across),
            pl.BlockSpec((utterances, frames, width), lambda i: (0, 0, 0)),
            pl.BlockSpec((utterances, slots, width), lambda i: (0, 0, 0)),
        ),
        scratch_shapes=[
            pltpu.VMEM((rows, tile), jnp.bfloat16),
            pltpu.VMEM((rows, width), jnp.float32),
        ],
        compiler_params=pltpu.CompilerParams(
            dimension_semantics=("arbitrary",), vmem_limit_bytes=VMEM_LIMIT
        ),
        name="backward",
    )(hidden, turned, w_out, bias, target, cells)


def local_sums(enc, pred, labels, frame_len, label_len, w_enc, w_pred, b_joint, w_out, b_out):
    utterances, frames, enc_dim = enc.shape
    slots = pred.shape[1]
    width = w_enc.shape[1]
    cells_count = utterances * slots * frames
    rows = (cells_count + LANES - 1) // LANES * LANES
    flat_enc = enc.reshape(utterances * frames, enc_dim)
    enc_proj = jnp.dot(flat_enc, w_enc, preferred_element_type=jnp.float32)
    pred_proj = jnp.einsum("bud,dj->buj", pred, w_pred, preferred_element_type=jnp.float32)
    pred_proj = pred_proj + b_joint.astype(jnp.float32)
    enc_proj = enc_proj.reshape(utterances, 1, frames, width)
    hidden = jnp.tanh(enc_proj + pred_proj[:, :, None, :]).astype(jnp.bfloat16)
    hidden = jnp.pad(hidden.reshape(cells_count, width), ((0, rows - cells_count), (0, 0)))
    hidden = lax.optimization_barrier(hidden)
    turned = hidden.T
    bias = b_out.astype(jnp.float32)[None, :]
    targets = jnp.concatenate([labels, jnp.ones((utterances, 1), jnp.int32)], axis=1)
    target = jnp.repeat(targets.reshape(-1), frames)
    target = jnp.pad(target, (0, rows - cells_count))[:, None]
    stats = row_stats(hidden, w_out, bias, target)
    grid_shape = (utterances, slots, frames)
    blank = stats[:cells_count, 1].reshape(grid_shape)
    emit = stats[:cells_count, 2].reshape(grid_shape)
    blank_occ, emit_occ, loss = lattice(blank, emit, frame_len, label_len)
    occ = jnp.stack([blank_occ.reshape(-1), emit_occ.reshape(-1)], axis=1)
    occ = jnp.pad(occ, ((0, rows - cells_count), (1, LANES - 3)))
    cells = jnp.where(jnp.arange(LANES)[None, :] == 0, stats, occ)
    grad_out, grad_bias_out, d_enc, d_pred = backward(
        hidden, turned, w_out, bias, target, cells, utterances, slots, frames
    )
    d_enc = d_enc.astype(jnp.bfloat16)
    d_pred = d_pred.astype(jnp.bfloat16)
    over_rows = (((0, 1), (0, 1)), ((), ()))
    grad_enc = lax.dot_general(enc, d_enc, over_rows, preferred_element_type=jnp.float32)
    grad_pred = lax.dot_general(pred, d_pred, over_rows, preferred_element_type=jnp.float32)
    grad_bias_joint = jnp.sum(d_pred.astype(jnp.float32), axis=(0, 1))
    return (jnp.sum(loss), (grad_enc, grad_pred, grad_out, grad_bias_out[0], grad_bias_joint))


def squares(items):
    total_sq = jnp.float32(0.0)
    for item in items:
        total_sq = total_sq + jnp.sum(item * item)
    return total_sq


def per_device(enc, pred, labels, frame_len, label_len, w_enc, w_pred, b_joint, w_out, b_out):
    loss_local, grads = local_sums(
        enc, pred, labels, frame_len, label_len, w_enc, w_pred, b_joint, w_out, b_out
    )
    count_local = jnp.sum(label_len).astype(jnp.float32)
    param_count = jnp.float32(w_enc.size + w_pred.size + w_out.size + b_out.size + b_joint.size)
    loss_total, label_total = lax.psum((loss_local, count_local), ("dp", "rep"))
    summed = lax.psum((grads[0], grads[1], grads[2], grads[3], grads[4]), ("dp", "rep"))
    scale = lax.rsqrt(squares(summed) / param_count + EPS)
    result = tuple((item * scale for item in summed))
    return (result[0], result[1], result[2], result[3], result[4], loss_total / label_total)


def solution(mesh):
    in_specs = (
        P(("dp", "rep"), None, None),
        P(("dp", "rep"), None, None),
        P(("dp", "rep"), None),
        P(("dp", "rep")),
        P(("dp", "rep")),
        P(),
        P(),
        P(),
        P(),
        P(),
    )
    out_specs = (P(), P(), P(), P(), P(), P())
    return jax.shard_map(
        per_device, mesh=mesh, in_specs=in_specs, out_specs=out_specs, check_vma=False
    )
```
